32 devices in a mesh: dp: 16 (over z, x, core), seq: 2 (over y).
Axes of the slice: x: 2, y: 2, z: 4, core: 2. Of those that a mesh axis runs over, the one named last changes fastest.
Arguments:
- frames: bfloat16 [16, 1024, 512], P('dp', 'seq'), may hold values from -6 to 6
- cotangent: bfloat16 [16, 1024, 512], P('dp', 'seq'), may hold values from -6 to 6
- weight_in: bfloat16 [2, 512, 2176], replicated, may hold values from -0.25 to 0.25
- qk_scales: float32 [2, 2, 128], replicated, may hold values from 0.5 to 1.5
- weight_out: bfloat16 [2, 1024, 512], replicated, may hold values from -0.1875 to 0.1875
- gains: float32 [2, 512], replicated, may hold values from 0.5 to 1.5
Outputs:
- output: bfloat16 [16, 1024, 512], P('dp', 'seq')
- grad_frames: bfloat16 [16, 1024, 512], P('dp', 'seq')
- grad_in: float32 [2, 512, 2176], P(None, 'dp')
- grad_out: float32 [2, 1024, 512], P(None, 'dp')
- grad_gains: float32 [2, 512], replicated
- grad_scales: float32 [2, 2, 128], replicated
The draws below stay inside these ranges and needn't reach their ends.
All inputs are finite; a program needn't handle non-finite values.
Results may differ from the reference program's by a relative error of at most 0.028.
Values may be sent and summed in bfloat16 or wider, within the bound.
A program may use at most 192 MiB of HBM per device.

```python
from functools import partial
import jax
import jax.numpy as jnp
from jax import lax

D = 512
E = 1024
S = 128
BLOCK = 256
NCH = 4
SEQLEN = 1024
BATCH = 16


def steps_of(own_key, extent, cuts, low, top_value):
    factor_of, own = 1.0, jax.random.fold_in(own_key, 6)
    for axis_at, shards_of in cuts:
        draws = jnp.exp(jax.random.uniform(jax.random.fold_in(own, axis_at), (shards_of,), jnp.float32, low / len(cuts), top_value / len(cuts)))
        factor_of = factor_of * jnp.repeat(draws, extent[axis_at] // shards_of).reshape([-1 if axis == axis_at else 1 for axis in range(len(extent))])
    return factor_of


def bell_draw(key, extent, scale, limit, cuts=(), held_as=jnp.bfloat16):
    entries = scale * jax.random.normal(key, extent, jnp.float32)
    if cuts:
        entries = entries * steps_of(key, extent, cuts, -0.22, 0.18)
    return jnp.clip(entries, -limit, limit).astype(held_as)


def setup_inputs(seed: int = 0) -> dict:
    key_list = jax.random.split(jax.random.key(seed), 7)
    frames = bell_draw(key_list[0], (BATCH, SEQLEN, D), 1.0, 6.0, ((0, 16), (1, 2)))
    cotangent = bell_draw(key_list[1], (BATCH, SEQLEN, D), 1.0, 6.0, ((0, 16), (1, 2)))
    weight_in = bell_draw(key_list[2], (2, D, 2 * E + S), D ** -0.5, 0.25)
    qk_scales = jnp.clip(1.0 + 0.1 * jax.random.normal(key_list[3], (2, 2, S), jnp.float32), 0.5, 1.5)
    weight_out = bell_draw(key_list[4], (2, E, D), E ** -0.5, 0.1875)
    gains = jnp.clip(1.0 + 0.1 * jax.random.normal(key_list[5], (2, D), jnp.float32), 0.5, 1.5)
    return dict(frames=frames, cotangent=cotangent, weight_in=weight_in, qk_scales=qk_scales, weight_out=weight_out, gains=gains)


EPSILON = 1e-06

def normed(values, gain_row):
    scaling = lax.rsqrt(lax.optimization_barrier(jnp.mean(values * values, axis=-1, keepdims=True)) + EPSILON)
    return values * scaling * gain_row

def mixer(projected, scale_pair, attend_axis):
    width = (projected.shape[-1] - scale_pair.shape[-1]) // 2
    active = jax.nn.silu(projected)
    gate_part = active[..., :width]
    value_part = active[..., width:2 * width].astype(jnp.bfloat16)
    shared = active[..., 2 * width:]
    query = (shared * scale_pair[0]).astype(jnp.bfloat16)
    keyed = (shared * scale_pair[1]).astype(jnp.bfloat16)
    length = projected.shape[attend_axis]
    if attend_axis == 1:
        score_form = 'gls,gms->glm'
        mix_form = 'glm,gme->gle'
    else:
        score_form = 'lgs,mgs->glm'
        mix_form = 'glm,mge->lge'
    scores = jnp.einsum(score_form, query.astype(jnp.float32), keyed.astype(jnp.float32))
    scores = scores * scale_pair.shape[-1] ** (-0.5)
    weights = (jnp.square(jax.nn.relu(scores)) / length).astype(jnp.bfloat16)
    mixed = jnp.einsum(mix_form, weights.astype(jnp.float32), value_part.astype(jnp.float32))
    return (gate_part * mixed).astype(jnp.bfloat16)

def rows_product(left, right):
    left_rows = left.reshape(-1, left.shape[-1])
    right_rows = right.reshape(-1, right.shape[-1])
    return lax.dot_general(left_rows, right_rows, (((0,), (0,)), ((), ())), preferred_element_type=jnp.float32)

def against(values, weight):
    return lax.dot_general(values, weight, (((values.ndim - 1,), (1,)), ((), ())), preferred_element_type=jnp.float32)

def unit_forward(inputs_now, weight_in, scale_pair, weight_out, gain_row, attend_axis):
    hidden = normed(inputs_now.astype(jnp.float32), gain_row).astype(jnp.bfloat16)
    projected = jnp.dot(hidden, weight_in, preferred_element_type=jnp.float32)
    gated = mixer(projected, scale_pair, attend_axis)
    result = (inputs_now.astype(jnp.float32) + jnp.dot(gated, weight_out, preferred_element_type=jnp.float32)).astype(jnp.bfloat16)
    return (result, (hidden, projected, gated))

def unit_backward(inputs_now, upstream, weight_in, scale_pair, weight_out, gain_row, saved, attend_axis):
    hidden, projected, gated = saved
    grad_out = rows_product(gated, upstream)
    grad_gated = against(upstream, weight_out).astype(jnp.bfloat16)
    pulled = jax.vjp(partial(mixer, attend_axis=attend_axis), projected, scale_pair)[1]
    grad_proj, grad_scale = pulled(grad_gated)
    grad_proj = grad_proj.astype(jnp.bfloat16)
    grad_in = rows_product(hidden, grad_proj)
    grad_hidden = against(grad_proj, weight_in)
    norm_pull = jax.vjp(normed, inputs_now.astype(jnp.float32), gain_row)[1]
    grad_inputs, grad_gain = norm_pull(grad_hidden)
    grad_inputs = (upstream.astype(jnp.float32) + grad_inputs).astype(jnp.bfloat16)
    return (grad_inputs, grad_in, grad_out, grad_gain, grad_scale)

def reference(frames, cotangent, weight_in, qk_scales, weight_out, gains):
    scaling = (BATCH * SEQLEN) ** (-0.5)

    def one_sequence(carry, pair):
        seq_frames, seq_cot = pair
        blocked = seq_frames.reshape(NCH, BLOCK, D)
        upstream = seq_cot.reshape(NCH, BLOCK, D)
        first, saved_first = unit_forward(blocked, weight_in[0], qk_scales[0], weight_out[0], gains[0], 1)
        second, saved_second = unit_forward(first, weight_in[1], qk_scales[1], weight_out[1], gains[1], 0)
        back_first, in_late, out_late, gain_late, scale_late = unit_backward(first, upstream, weight_in[1], qk_scales[1], weight_out[1], gains[1], saved_second, 0)
        back_frames, in_early, out_early, gain_early, scale_early = unit_backward(blocked, back_first, weight_in[0], qk_scales[0], weight_out[0], gains[0], saved_first, 1)
        carry = (carry[0] + jnp.stack([in_early, in_late]), carry[1] + jnp.stack([out_early, out_late]), carry[2] + jnp.stack([gain_early, gain_late]), carry[3] + jnp.stack([scale_early, scale_late]))
        return (carry, (second.reshape(SEQLEN, D), back_frames.reshape(SEQLEN, D)))
    start = (jnp.zeros((2, D, 2 * E + S), jnp.float32), jnp.zeros((2, E, D), jnp.float32), jnp.zeros((2, D), jnp.float32), jnp.zeros((2, 2, S), jnp.float32))
    totals, outs_pair = lax.scan(one_sequence, start, (frames, cotangent))
    return (outs_pair[0], outs_pair[1], totals[0] * scaling, totals[1] * scaling, totals[2] * scaling, totals[3] * scaling)
```

```python
from functools import partial

import jax
import jax.numpy as jnp
from jax import lax
from jax.sharding import PartitionSpec as P

BLOCK = 256


EPSILON = 1e-06


def normed(values, gain_row):
    scaling = lax.rsqrt(jnp.mean(values * values, axis=-1, keepdims=True) + EPSILON)
    return values * scaling * gain_row


def mixer(projected, scale_pair, attend_axis):
    width = (projected.shape[-1] - scale_pair.shape[-1]) // 2
    active = jax.nn.silu(projected)
    gate_part = active[..., :width]
    value_part = active[..., width : 2 * width].astype(jnp.bfloat16)
    shared = active[..., 2 * width :]
    query = (shared * scale_pair[0]).astype(jnp.bfloat16)
    keyed = (shared * scale_pair[1]).astype(jnp.bfloat16)
    length = projected.shape[attend_axis]
    if attend_axis == 1:
        score_form = "gls,gms->glm"
        mix_form = "glm,gme->gle"
    else:
        score_form = "lgs,mgs->glm"
        mix_form = "glm,mge->lge"
    scores = jnp.einsum(score_form, query, keyed, preferred_element_type=jnp.float32)
    scores = scores * scale_pair.shape[-1] ** (-0.5)
    weights = (jnp.square(jax.nn.relu(scores)) / length).astype(jnp.bfloat16)
    mixed = jnp.einsum(mix_form, weights, value_part, preferred_element_type=jnp.float32)
    return (gate_part * mixed).astype(jnp.bfloat16)


def rows_product(left, right):
    left_rows = left.reshape(-1, left.shape[-1])
    right_rows = right.reshape(-1, right.shape[-1])
    return lax.dot_general(
        left_rows, right_rows, (((0,), (0,)), ((), ())), preferred_element_type=jnp.float32
    )


def against(values, weight):
    return lax.dot_general(
        values, weight, (((values.ndim - 1,), (1,)), ((), ())), preferred_element_type=jnp.float32
    )


def unit_forward(inputs_now, weight_in, scale_pair, weight_out, gain_row, attend_axis):
    hidden = normed(inputs_now.astype(jnp.float32), gain_row).astype(jnp.bfloat16)
    projected = jnp.dot(hidden, weight_in, preferred_element_type=jnp.float32)
    gated = mixer(projected, scale_pair, attend_axis)
    result = (
        inputs_now.astype(jnp.float32)
        + jnp.dot(gated, weight_out, preferred_element_type=jnp.float32)
    ).astype(jnp.bfloat16)
    return (result, (hidden, projected, gated))


def unit_backward(
    inputs_now, upstream, weight_in, scale_pair, weight_out, gain_row, saved, attend_axis
):
    hidden, projected, gated = saved
    grad_out = rows_product(gated, upstream)
    grad_gated = against(upstream, weight_out).astype(jnp.bfloat16)
    pulled = jax.vjp(partial(mixer, attend_axis=attend_axis), projected, scale_pair)[1]
    grad_proj, grad_scale = pulled(grad_gated)
    grad_proj = grad_proj.astype(jnp.bfloat16)
    grad_in = rows_product(hidden, grad_proj)
    grad_hidden = against(grad_proj, weight_in)
    norm_pull = jax.vjp(normed, inputs_now.astype(jnp.float32), gain_row)[1]
    grad_inputs, grad_gain = norm_pull(grad_hidden)
    grad_inputs = (upstream.astype(jnp.float32) + grad_inputs).astype(jnp.bfloat16)
    return (grad_inputs, grad_in, grad_out, grad_gain, grad_scale)


def bit_of(axis, bit):
    return lax.rem(lax.axis_index(axis) // (1 << bit), 2)


def partner_swap(value, axis, bit):
    size = lax.axis_size(axis)
    return lax.ppermute(value, axis, [(i, i ^ (1 << bit)) for i in range(size)])


def axis_bits(axis):
    return [(axis, bit) for bit in range(lax.axis_size(axis).bit_length() - 1)]


def halving_order(turn):
    dp_bits, seq_bits = axis_bits("dp"), axis_bits("seq")
    rest = dp_bits[1:2] + seq_bits + dp_bits[2:]
    turn = turn % max(len(rest), 1)
    return dp_bits[:1] + rest[turn:] + rest[:turn]


def pick(value, place, at):
    return lax.dynamic_index_in_dim(value, at, place, keepdims=False)


def shared_sum(partial, turn):
    rows, columns = partial.shape
    dp_bits, seq_bits = axis_bits("dp"), axis_bits("seq")
    left = dp_bits[::-1] + seq_bits[::-1]
    inner = rows >> len(left)
    held = partial.reshape((2,) * len(left) + (inner, columns))
    for axis, bit in halving_order(turn):
        place = left.index((axis, bit))
        left.pop(place)
        mine = bit_of(axis, bit)
        got = partner_swap(pick(held, place, 1 - mine), axis, bit)
        kept = pick(held, place, mine)
        held = (kept.astype(jnp.float32) + got.astype(jnp.float32)).astype(jnp.bfloat16)
    for axis, bit in seq_bits:
        held = held.reshape(-1, columns)
        got = partner_swap(held, axis, bit)
        mine = bit_of(axis, bit)
        held = jnp.concatenate(
            [jnp.where(mine == 0, held, got), jnp.where(mine == 0, got, held)], axis=0
        )
    return held.reshape(-1, columns)


def full_sum(value):
    for axis, bit in axis_bits("dp") + axis_bits("seq"):
        value = value + partner_swap(value, axis, bit)
    return value


def exchange(value, split, join):
    count = lax.axis_size("seq")
    me = lax.axis_index("seq")
    piece = value.shape[split] // count
    width = value.shape[join]
    shape = list(value.shape)
    shape[split] = piece
    shape[join] = width * count
    out = jnp.zeros(shape, value.dtype)
    for step in range(count):
        other = jnp.bitwise_xor(me, step)
        part = lax.dynamic_slice_in_dim(value, other * piece, piece, split)
        if step:
            part = lax.ppermute(part, "seq", [(i, i ^ step) for i in range(count)])
        out = lax.dynamic_update_slice_in_dim(out, part, other * width, join)
    return out


def column_cuts(columns, parts):
    lanes = columns // 128
    ends = [128 * ((lanes * (i + 1)) // parts) for i in range(parts)]
    return list(zip([0] + ends[:-1], ends))


def on_device(frames, cotangent, weight_in, qk_scales, weight_out, gains):
    block_count = frames.shape[1] // BLOCK
    width = frames.shape[2]
    tokens_all = frames.shape[0] * frames.shape[1] * lax.axis_size("dp") * lax.axis_size("seq")
    scaling = tokens_all ** (-0.5)
    blocked = frames.reshape(-1, BLOCK, width)
    upstream = exchange(cotangent.reshape(block_count, BLOCK, width), 1, 0)
    first, saved_first = unit_forward(
        blocked, weight_in[0], qk_scales[0], weight_out[0], gains[0], 1
    )
    first_pos = exchange(first, 1, 0)
    second, saved_second = unit_forward(
        first_pos, weight_in[1], qk_scales[1], weight_out[1], gains[1], 0
    )
    result = exchange(second, 0, 1)
    back_pos, in_late, out_late, gain_late, scale_late = unit_backward(
        first_pos, upstream, weight_in[1], qk_scales[1], weight_out[1], gains[1], saved_second, 0
    )
    back_first = exchange(back_pos, 0, 1)
    back_frames, in_early, out_early, gain_early, scale_early = unit_backward(
        blocked, back_first, weight_in[0], qk_scales[0], weight_out[0], gains[0], saved_first, 1
    )

    def summed(partial, parts, turn):
        partial = partial.astype(jnp.bfloat16)
        pieces = [
            shared_sum(partial[:, low:high], turn + index)
            for index, (low, high) in enumerate(column_cuts(partial.shape[1], parts))
        ]
        return jnp.concatenate(pieces, axis=1).astype(jnp.float32) * scaling

    out_sum = [summed(out_early, 1, 0), summed(out_late, 1, 2)]
    in_sum = [summed(in_early, 3, 0), summed(in_late, 2, 0)]
    packed = jnp.concatenate(
        [gain_early, gain_late, scale_early.reshape(-1), scale_late.reshape(-1)]
    )
    small = full_sum(packed) * scaling
    return (
        result.reshape(frames.shape),
        back_frames.reshape(frames.shape),
        jnp.stack(in_sum),
        jnp.stack(out_sum),
        small[: 2 * width].reshape(2, width),
        small[2 * width :].reshape(qk_scales.shape),
    )


def solution(mesh):
    in_specs = (P("dp", "seq", None), P("dp", "seq", None), P(), P(), P(), P())
    out_specs = (
        P("dp", "seq", None),
        P("dp", "seq", None),
        P(None, "dp", None),
        P(None, "dp", None),
        P(),
        P(),
    )
    return jax.shard_map(
        on_device, mesh=mesh, in_specs=in_specs, out_specs=out_specs, check_vma=False
    )
```

```python
from functools import partial
from functools import partial as partial_of

import jax
import jax.numpy as jnp
from jax import lax
from jax.experimental import pallas as pl
from jax.experimental.pallas import tpu as pltpu
from jax.sharding import PartitionSpec as P

BLOCK = 256


EPSILON = 1e-06


def normed(values, gain_row):
    scaling = lax.rsqrt(jnp.mean(values * values, axis=-1, keepdims=True) + EPSILON)
    return values * scaling * gain_row


def mixer(projected, scale_pair, attend_axis):
    width = (projected.shape[-1] - scale_pair.shape[-1]) // 2
    active = jax.nn.silu(projected)
    gate_part = active[..., :width]
    value_part = active[..., width : 2 * width].astype(jnp.bfloat16)
    shared = active[..., 2 * width :]
    query = (shared * scale_pair[0]).astype(jnp.bfloat16)
    keyed = (shared * scale_pair[1]).astype(jnp.bfloat16)
    length = projected.shape[attend_axis]
    if attend_axis == 1:
        score_form = "gls,gms->glm"
        mix_form = "glm,gme->gle"
    else:
        score_form = "lgs,mgs->glm"
        mix_form = "glm,mge->lge"
    scores = jnp.einsum(score_form, query, keyed, preferred_element_type=jnp.float32)
    scores = scores * scale_pair.shape[-1] ** (-0.5)
    weights = (jnp.square(jax.nn.relu(scores)) / length).astype(jnp.bfloat16)
    mixed = jnp.einsum(mix_form, weights, value_part, preferred_element_type=jnp.float32)
    return (gate_part * mixed).astype(jnp.bfloat16)


def rows_product(left, right):
    left_rows = left.reshape(-1, left.shape[-1])
    right_rows = right.reshape(-1, right.shape[-1])
    return lax.dot_general(
        left_rows, right_rows, (((0,), (0,)), ((), ())), preferred_element_type=jnp.float32
    )


def against(values, weight):
    return lax.dot_general(
        values, weight, (((values.ndim - 1,), (1,)), ((), ())), preferred_element_type=jnp.float32
    )


def unit_forward(inputs_now, weight_in, scale_pair, weight_out, gain_row, attend_axis):
    hidden = normed(inputs_now.astype(jnp.float32), gain_row).astype(jnp.bfloat16)
    projected = jnp.dot(hidden, weight_in, preferred_element_type=jnp.float32)
    gated = mixer(projected, scale_pair, attend_axis)
    result = (
        inputs_now.astype(jnp.float32)
        + jnp.dot(gated, weight_out, preferred_element_type=jnp.float32)
    ).astype(jnp.bfloat16)
    return (result, (hidden, projected, gated))


def unit_backward(
    inputs_now, upstream, weight_in, scale_pair, weight_out, gain_row, saved, attend_axis
):
    hidden, projected, gated = saved
    grad_out = rows_product(gated, upstream)
    grad_gated = against(upstream, weight_out).astype(jnp.bfloat16)
    pulled = jax.vjp(partial(mixer, attend_axis=attend_axis), projected, scale_pair)[1]
    grad_proj, grad_scale = pulled(grad_gated)
    grad_proj = grad_proj.astype(jnp.bfloat16)
    grad_in = rows_product(hidden, grad_proj)
    grad_hidden = against(grad_proj, weight_in)
    norm_pull = jax.vjp(normed, inputs_now.astype(jnp.float32), gain_row)[1]
    grad_inputs, grad_gain = norm_pull(grad_hidden)
    grad_inputs = (upstream.astype(jnp.float32) + grad_inputs).astype(jnp.bfloat16)
    return (grad_inputs, grad_in, grad_out, grad_gain, grad_scale)


def bit_of(axis, bit):
    return lax.rem(lax.axis_index(axis) // (1 << bit), 2)


def axis_bits(axis):
    return [(axis, bit) for bit in range(lax.axis_size(axis).bit_length() - 1)]


def partner(axis, bit):
    spot = {name: lax.axis_index(name) for name in ("dp", "seq")}
    spot[axis] = spot[axis] + (1 << bit) * (1 - 2 * bit_of(axis, bit))
    return (spot["dp"], spot["seq"])


def halving_order(turn):
    dp_bits, seq_bits = axis_bits("dp"), axis_bits("seq")
    rest = dp_bits[1:2] + seq_bits + dp_bits[2:-1]
    turn = turn % max(len(rest), 1)
    return dp_bits[:1] + rest[turn:] + rest[:turn] + dp_bits[2:][-1:]


def place_of(known, leading):
    return tuple(known.get(bit, slice(None)) for bit in leading)


def gradient_kernel(plan, scaling, count_in, *refs):
    dp_bits, seq_bits = axis_bits("dp"), axis_bits("seq")
    leading = dp_bits[::-1] + seq_bits[::-1]
    steps = len(leading)
    given, small = refs[:count_in], refs[count_in]
    results, small_out = refs[count_in + 1 : 2 * count_in + 1], refs[2 * count_in + 1]
    scratch = list(refs[2 * count_in + 2 :])
    small_held, small_got, send_sems, recv_sems = scratch[:4]
    scratch = scratch[4:]
    total = len(plan)
    accs, scratch = scratch[:total], scratch[total:]
    gathers, scratch = scratch[:total], scratch[total:]
    landings = [scratch[steps * i : steps * (i + 1)] for i in range(total)]
    mine = {bit: bit_of(*bit) for bit in leading}
    where = {bit: partner(*bit) for bit in leading}
    barrier = pltpu.get_barrier_semaphore()
    for bit in leading:
        pl.semaphore_signal(
            barrier, inc=1, device_id=where[bit], device_id_type=pl.DeviceIdType.MESH
        )
    pl.semaphore_wait(barrier, steps)
    started = []

    def send(source, target, row, column, bit):
        copy = pltpu.make_async_remote_copy(
            src_ref=source,
            dst_ref=target,
            send_sem=send_sems.at[row, column],
            recv_sem=recv_sems.at[row, column],
            device_id=where[bit],
            device_id_type=pl.DeviceIdType.MESH,
        )
        copy.start()
        started.append(copy)
        return copy

    orders = [halving_order(turn) for _, _, _, turn in plan]
    flying = [None] * total
    known = [{} for _ in plan]

    def launch(index, step):
        array, low, high, _ = plan[index]
        bit = orders[index][step]
        if step == 0:
            left = leading
            place = place_of({bit: 1 - mine[bit]}, left)
            source = given[array].at[place + (slice(None), slice(low, high))]
        else:
            left = [other for other in leading if other != orders[index][0]]
            place = place_of({**known[index], bit: 1 - mine[bit]}, left)
            source = accs[index].at[place]
        flying[index] = send(source, landings[index][step], index, step, bit)

    for index in range(total):
        launch(index, 0)
    small_held[0] = small[...]
    small_flying = send(small_held.at[0], small_got.at[0], total, 0, leading[0])
    for step in range(steps):
        for index in range(total):
            array, low, high, _ = plan[index]
            bit = orders[index][step]
            flying[index].wait_recv()
            landed = landings[index][step]
            if step == 0:
                place = place_of({bit: mine[bit]}, leading)
                accs[index][...] = (
                    given[array][place + (slice(None), slice(low, high))] + landed[...]
                )
            else:
                known[index][bit] = mine[bit]
                left = [other for other in leading if other != orders[index][0]]
                place = place_of(known[index], left)
                accs[index][place] = accs[index][place] + landed[...]
            if step + 1 < steps:
                launch(index, step + 1)
            else:
                left = [other for other in leading if other != orders[index][0]]
                gathers[index][place_of(mine, seq_bits)] = accs[index][place_of(mine, left)]
                if seq_bits:
                    spot = gathers[index].at[place_of(mine, seq_bits)]
                    flying[index] = send(spot, spot, index, steps, seq_bits[0])
        small_flying.wait_recv()
        small_held[step + 1] = small_held[step] + small_got[step]
        if step + 1 < steps:
            small_flying = send(
                small_held.at[step + 1],
                small_got.at[step + 1],
                total,
                step + 1,
                leading[step + 1],
            )
    small_out[...] = small_held[steps] * scaling
    for turn in range(1, len(seq_bits)):
        for index in range(total):
            flying[index].wait_recv()
            have = {bit: mine[bit] for bit in seq_bits[turn:]}
            spot = gathers[index].at[place_of(have, seq_bits)]
            flying[index] = send(spot, spot, index, steps + turn, seq_bits[turn])
    for index in range(total):
        array, low, high, _ = plan[index]
        if seq_bits:
            flying[index].wait_recv()
        inner = gathers[index].shape[-2]
        for part in range(1 << len(seq_bits)):
            spot = tuple((part >> bit) % 2 for _, bit in seq_bits)
            results[array][part, :, low:high] = (
                gathers[index][spot].astype(jnp.float32) * scaling
            )
    for copy in started:
        copy.wait_send()


def reduced(partials, cuts, small, scaling):
    dp_bits, seq_bits = axis_bits("dp"), axis_bits("seq")
    steps = len(dp_bits) + len(seq_bits)
    shaped, shapes, accs, gathers, landings = [], [], [], [], []
    for partial in partials:
        rows, columns = partial.shape
        inner = rows >> steps
        shaped.append(partial.reshape((2,) * steps + (inner, columns)))
        shapes.append(
            jax.ShapeDtypeStruct((1 << len(seq_bits), inner, columns), jnp.float32)
        )
    for array, low, high, _ in cuts:
        tail = (shaped[array].shape[-2], high - low)
        accs.append(pltpu.VMEM((2,) * (steps - 1) + tail, jnp.bfloat16))
        gathers.append(pltpu.VMEM((2,) * len(seq_bits) + tail, jnp.bfloat16))
        landings += [
            pltpu.VMEM((2,) * (steps - 1 - step) + tail, jnp.bfloat16) for step in range(steps)
        ]
    lines = small.reshape(-1, 128)
    sems = pltpu.SemaphoreType.DMA((len(cuts) + 1, steps + len(seq_bits)))
    space = pl.BlockSpec(memory_space=pltpu.VMEM)
    made = pl.pallas_call(
        partial_of(gradient_kernel, cuts, scaling, len(partials)),
        out_shape=shapes + [jax.ShapeDtypeStruct(lines.shape, jnp.float32)],
        in_specs=[space] * (len(partials) + 1),
        out_specs=[space] * (len(partials) + 1),
        scratch_shapes=[
            pltpu.VMEM((steps + 1,) + lines.shape, jnp.float32),
            pltpu.VMEM((steps,) + lines.shape, jnp.float32),
            sems,
            sems,
        ]
        + accs
        + gathers
        + landings,
        compiler_params=pltpu.CompilerParams(
            collective_id=0, has_side_effects=True, vmem_limit_bytes=48 << 20
        ),
        name="gradient_sums",
    )(*shaped, lines)
    sums = [value.reshape(-1, value.shape[-1]) for value in made[:-1]]
    return sums, made[-1].reshape(-1)


def exchange(value, split, join):
    count = lax.axis_size("seq")
    me = lax.axis_index("seq")
    piece = value.shape[split] // count
    width = value.shape[join]
    shape = list(value.shape)
    shape[split] = piece
    shape[join] = width * count
    out = jnp.zeros(shape, value.dtype)
    for step in range(count):
        other = jnp.bitwise_xor(me, step)
        part = lax.dynamic_slice_in_dim(value, other * piece, piece, split)
        if step:
            part = lax.ppermute(part, "seq", [(i, i ^ step) for i in range(count)])
        out = lax.dynamic_update_slice_in_dim(out, part, other * width, join)
    return out


def column_cuts(columns, parts):
    lanes = columns // 128
    ends = [128 * ((lanes * (i + 1)) // parts) for i in range(parts)]
    return list(zip([0] + ends[:-1], ends))


def on_device(frames, cotangent, weight_in, qk_scales, weight_out, gains):
    block_count = frames.shape[1] // BLOCK
    width = frames.shape[2]
    tokens_all = frames.shape[0] * frames.shape[1] * lax.axis_size("dp") * lax.axis_size("seq")
    scaling = tokens_all ** (-0.5)
    blocked = frames.reshape(-1, BLOCK, width)
    upstream = exchange(cotangent.reshape(block_count, BLOCK, width), 1, 0)
    first, saved_first = unit_forward(
        blocked, weight_in[0], qk_scales[0], weight_out[0], gains[0], 1
    )
    first_pos = exchange(first, 1, 0)
    second, saved_second = unit_forward(
        first_pos, weight_in[1], qk_scales[1], weight_out[1], gains[1], 0
    )
    result = exchange(second, 0, 1)
    back_pos, in_late, out_late, gain_late, scale_late = unit_backward(
        first_pos, upstream, weight_in[1], qk_scales[1], weight_out[1], gains[1], saved_second, 0
    )
    back_first = exchange(back_pos, 0, 1)
    back_frames, in_early, out_early, gain_early, scale_early = unit_backward(
        blocked, back_first, weight_in[0], qk_scales[0], weight_out[0], gains[0], saved_first, 1
    )

    grads = [
        value.astype(jnp.bfloat16) for value in (in_late, out_late, out_early, in_early)
    ]
    packed = jnp.concatenate(
        [gain_early, gain_late, scale_early.reshape(-1), scale_late.reshape(-1)]
    )
    cuts = []
    for array, (parts, turn) in enumerate(((3, 0), (3, 1), (2, 0), (3, 0))):
        for index, (low, high) in enumerate(column_cuts(grads[array].shape[1], parts)):
            cuts.append((array, low, high, turn + index))
    sums, small = reduced(grads, cuts, packed, scaling)
    in_sum, out_sum = [sums[3], sums[0]], [sums[2], sums[1]]
    return (
        result.reshape(frames.shape),
        back_frames.reshape(frames.shape),
        jnp.stack(in_sum),
        jnp.stack(out_sum),
        small[: 2 * width].reshape(2, width),
        small[2 * width :].reshape(qk_scales.shape),
    )


def solution(mesh):
    in_specs = (P("dp", "seq", None), P("dp", "seq", None), P(), P(), P(), P())
    out_specs = (
        P("dp", "seq", None),
        P("dp", "seq", None),
        P(None, "dp", None),
        P(None, "dp", None),
        P(),
        P(),
    )
    return jax.shard_map(
        on_device, mesh=mesh, in_specs=in_specs, out_specs=out_specs, check_vma=False
    )
```

```python
from functools import partial
from functools import partial as partial_of

import jax
import jax.numpy as jnp
from jax import lax
from jax.experimental import pallas as pl
from jax.experimental.pallas import tpu as pltpu
from jax.sharding import PartitionSpec as P

BLOCK = 256


EPSILON = 1e-06


def normed(values, gain_row):
    scaling = lax.rsqrt(jnp.mean(values * values, axis=-1, keepdims=True) + EPSILON)
    return values * scaling * gain_row


def mixer(projected, scale_pair, attend_axis):
    width = (projected.shape[-1] - scale_pair.shape[-1]) // 2
    active = jax.nn.silu(projected)
    gate_part = active[..., :width]
    value_part = active[..., width : 2 * width].astype(jnp.bfloat16)
    shared = active[..., 2 * width :]
    query = (shared * scale_pair[0]).astype(jnp.bfloat16)
    keyed = (shared * scale_pair[1]).astype(jnp.bfloat16)
    length = projected.shape[attend_axis]
    if attend_axis == 1:
        score_form = "gls,gms->glm"
        mix_form = "glm,gme->gle"
    else:
        score_form = "lgs,mgs->glm"
        mix_form = "glm,mge->lge"
    scores = jnp.einsum(score_form, query, keyed, preferred_element_type=jnp.float32)
    scores = scores * scale_pair.shape[-1] ** (-0.5)
    weights = (jnp.square(jax.nn.relu(scores)) / length).astype(jnp.bfloat16)
    mixed = jnp.einsum(mix_form, weights, value_part, preferred_element_type=jnp.float32)
    return (gate_part * mixed).astype(jnp.bfloat16)


def rows_product(left, right):
    left_rows = left.reshape(-1, left.shape[-1])
    right_rows = right.reshape(-1, right.shape[-1])
    return lax.dot_general(
        left_rows, right_rows, (((0,), (0,)), ((), ())), preferred_element_type=jnp.float32
    )


def against(values, weight):
    return lax.dot_general(
        values, weight, (((values.ndim - 1,), (1,)), ((), ())), preferred_element_type=jnp.float32
    )


def unit_forward(inputs_now, weight_in, scale_pair, weight_out, gain_row, attend_axis):
    hidden = normed(inputs_now.astype(jnp.float32), gain_row).astype(jnp.bfloat16)
    projected = jnp.dot(hidden, weight_in, preferred_element_type=jnp.float32)
    gated = mixer(projected, scale_pair, attend_axis)
    result = (
        inputs_now.astype(jnp.float32)
        + jnp.dot(gated, weight_out, preferred_element_type=jnp.float32)
    ).astype(jnp.bfloat16)
    return (result, (hidden, projected, gated))


def unit_backward(
    inputs_now, upstream, weight_in, scale_pair, weight_out, gain_row, saved, attend_axis
):
    hidden, projected, gated = saved
    grad_out = rows_product(gated, upstream)
    grad_gated = against(upstream, weight_out).astype(jnp.bfloat16)
    pulled = jax.vjp(partial(mixer, attend_axis=attend_axis), projected, scale_pair)[1]
    grad_proj, grad_scale = pulled(grad_gated)
    grad_proj = grad_proj.astype(jnp.bfloat16)
    grad_in = rows_product(hidden, grad_proj)
    grad_hidden = against(grad_proj, weight_in)
    norm_pull = jax.vjp(normed, inputs_now.astype(jnp.float32), gain_row)[1]
    grad_inputs, grad_gain = norm_pull(grad_hidden)
    grad_inputs = (upstream.astype(jnp.float32) + grad_inputs).astype(jnp.bfloat16)
    return (grad_inputs, grad_in, grad_out, grad_gain, grad_scale)


def bit_of(axis, bit):
    return lax.rem(lax.axis_index(axis) // (1 << bit), 2)


def axis_bits(axis):
    return [(axis, bit) for bit in range(lax.axis_size(axis).bit_length() - 1)]


def partner(axis, bit):
    spot = {name: lax.axis_index(name) for name in ("dp", "seq")}
    spot[axis] = spot[axis] + (1 << bit) * (1 - 2 * bit_of(axis, bit))
    return (spot["dp"], spot["seq"])


def halving_order(turn):
    dp_bits, seq_bits = axis_bits("dp"), axis_bits("seq")
    rest = dp_bits[1:2] + seq_bits + dp_bits[2:-1]
    turn = turn % max(len(rest), 1)
    return dp_bits[:1] + rest[turn:] + rest[:turn] + dp_bits[2:][-1:]


def place_of(known, leading):
    return tuple(known.get(bit, slice(None)) for bit in leading)


def gradient_kernel(plan, scaling, count_in, block, count_held, *refs):
    dp_bits, seq_bits = axis_bits("dp"), axis_bits("seq")
    leading = dp_bits[::-1] + seq_bits[::-1]
    steps = len(leading)
    given, small = list(refs[:count_in]), refs[count_in]
    refs = list(refs[count_in + 1 :])
    held_in, refs = refs[:count_held], refs[count_held:]
    arrays = count_in + (2 if block else 0)
    results, small_out = refs[:arrays], refs[arrays]
    scratch = refs[arrays + 1 :]
    if block:
        back_ref, out_grad, in_grad, proj_grad, small_all = (
            scratch[0], scratch[-4], scratch[-3], scratch[-2], scratch[-1]
        )
        given += [out_grad, in_grad]
        scratch = scratch[1:-4]
    small_held, small_got, send_sems, recv_sems = scratch[:4]
    scratch = scratch[4:]
    total = len(plan)
    accs, scratch = scratch[:total], scratch[total:]
    gathers, scratch = scratch[:total], scratch[total:]
    landings = [scratch[steps * i : steps * (i + 1)] for i in range(total)]
    mine = {bit: bit_of(*bit) for bit in leading}
    where = {bit: partner(*bit) for bit in leading}
    barrier = pltpu.get_barrier_semaphore()
    for bit in leading:
        pl.semaphore_signal(
            barrier, inc=1, device_id=where[bit], device_id_type=pl.DeviceIdType.MESH
        )
    pl.semaphore_wait(barrier, steps)
    started = []

    def send(source, target, row, column, bit):
        copy = pltpu.make_async_remote_copy(
            src_ref=source,
            dst_ref=target,
            send_sem=send_sems.at[row, column],
            recv_sem=recv_sems.at[row, column],
            device_id=where[bit],
            device_id_type=pl.DeviceIdType.MESH,
        )
        copy.start()
        started.append(copy)
        return copy

    orders = [halving_order(turn) for _, _, _, turn in plan]
    flying = [None] * total
    known = [{} for _ in plan]

    def launch(index, step):
        array, low, high, _ = plan[index]
        bit = orders[index][step]
        if step == 0:
            left = leading
            place = place_of({bit: 1 - mine[bit]}, left)
            source = given[array].at[place + (slice(None), slice(low, high))]
        else:
            left = [other for other in leading if other != orders[index][0]]
            place = place_of({**known[index], bit: 1 - mine[bit]}, left)
            source = accs[index].at[place]
        flying[index] = send(source, landings[index][step], index, step, bit)

    at_step = [0] * total
    small_state = {"step": 0}

    def advance(index):
        step = at_step[index]
        if step >= steps:
            return
        array, low, high, _ = plan[index]
        bit = orders[index][step]
        flying[index].wait_recv()
        landed = landings[index][step]
        left = [other for other in leading if other != orders[index][0]]
        if step == 0:
            place = place_of({bit: mine[bit]}, leading)
            accs[index][...] = given[array][place + (slice(None), slice(low, high))] + landed[...]
        else:
            known[index][bit] = mine[bit]
            place = place_of(known[index], left)
            accs[index][place] = accs[index][place] + landed[...]
        at_step[index] = step + 1
        if step + 1 < steps:
            launch(index, step + 1)
        else:
            gathers[index][place_of(mine, seq_bits)] = accs[index][place_of(mine, left)]
            if seq_bits:
                spot = gathers[index].at[place_of(mine, seq_bits)]
                flying[index] = send(spot, spot, index, steps, seq_bits[0])

    def small_send():
        step = small_state["step"]
        small_state["copy"] = send(
            small_held.at[step], small_got.at[step], total, step, leading[step]
        )

    def small_advance():
        step = small_state["step"]
        if step >= steps:
            return
        small_state["copy"].wait_recv()
        small_held[step + 1] = small_held[step] + small_got[step]
        small_state["step"] = step + 1
        if step + 1 < steps:
            small_send()

    def of_arrays(*wanted):
        return [index for index in range(total) if plan[index][0] in wanted]

    def advance_all(*wanted):
        for index in of_arrays(*wanted):
            advance(index)

    def launch_all(*wanted):
        for index in of_arrays(*wanted):
            launch(index, 0)

    if block:
        late = tuple(range(count_in))
        out_at, in_at = count_in, count_in + 1
        launch_all(*late)
        block_backward(
            block,
            held_in,
            (back_ref, out_grad, in_grad, proj_grad, small_all),
            small,
            (
                lambda: launch_all(out_at),
                lambda: advance_all(*late, out_at),
                lambda: launch_all(in_at),
            ),
        )
        small_held[0] = small_all[...]
    else:
        launch_all(*range(count_in))
        small_held[0] = small[...]
    small_send()
    while min(at_step) < steps:
        if block:
            advance_all(in_at)
            advance_all(*late, out_at)
        else:
            advance_all(*range(count_in))
        small_advance()
    while small_state["step"] < steps:
        small_advance()
    small_out[...] = small_held[steps] * scaling
    for turn in range(1, len(seq_bits)):
        for index in range(total):
            flying[index].wait_recv()
            have = {bit: mine[bit] for bit in seq_bits[turn:]}
            spot = gathers[index].at[place_of(have, seq_bits)]
            flying[index] = send(spot, spot, index, steps + turn, seq_bits[turn])
    for index in range(total):
        array, low, high, _ = plan[index]
        if seq_bits:
            flying[index].wait_recv()
        inner = gathers[index].shape[-2]
        for part in range(1 << len(seq_bits)):
            spot = tuple((part >> bit) % 2 for _, bit in seq_bits)
            results[array][part, :, low:high] = (
                gathers[index][spot].astype(jnp.float32) * scaling
            )
    for copy in started:
        copy.wait_send()


def dot_nt(left, right):
    return lax.dot_general(
        left, right, (((1,), (1,)), ((), ())), preferred_element_type=jnp.float32
    )


def dot_tn(left, right):
    return lax.dot_general(
        left, right, (((0,), (0,)), ((), ())), preferred_element_type=jnp.float32
    )


def silu_pair(values):
    sigmoid = 1.0 / (1.0 + jnp.exp(-values))
    active = values * sigmoid
    return active, sigmoid + active * (1.0 - sigmoid)


def store_rows(target, value, low, high):
    lead = target.shape[:-2]
    target[(slice(None),) * (len(lead) + 1) + (slice(low, high),)] = value.astype(
        jnp.bfloat16
    ).reshape(lead + (target.shape[-2], high - low))


def block_backward(length, held_in, made, small, hooks):
    x_ref, up_ref, hidden_ref, proj_ref, gated_ref, win_ref, wout_ref, scale_ref, gain_ref = held_in
    back_ref, out_grad, in_grad, proj_grad, small_all = made
    out_ready, between, in_ready = hooks
    frames, columns = proj_ref.shape
    shared = scale_ref.shape[-1]
    width = (columns - shared) // 2
    store_rows(out_grad, dot_tn(gated_ref[...], up_ref[...]), 0, up_ref.shape[-1])
    out_ready()
    between()
    root = shared ** (-0.5)
    first_scale, second_scale = scale_ref[0:1], scale_ref[1:2]
    scale_sums = [0.0, 0.0]
    for low in range(0, frames, length):
        rows = slice(low, low + length)
        grad_gated = dot_nt(up_ref[rows], wout_ref[...]).astype(jnp.bfloat16).astype(jnp.float32)
        mixed_in, mixed_slope = silu_pair(proj_ref[rows, 2 * width :])
        query = (mixed_in * first_scale).astype(jnp.bfloat16)
        keyed = (mixed_in * second_scale).astype(jnp.bfloat16)
        value, value_slope = silu_pair(proj_ref[rows, width : 2 * width])
        value = value.astype(jnp.bfloat16)
        raised = jnp.maximum(dot_nt(query, keyed) * root, 0.0)
        weights = (raised * raised / length).astype(jnp.bfloat16)
        mixed = jnp.dot(weights, value, preferred_element_type=jnp.float32)
        gate, gate_slope = silu_pair(proj_ref[rows, :width])
        proj_grad[rows, :width] = (grad_gated * mixed * gate_slope).astype(jnp.bfloat16)
        grad_mixed = (grad_gated * gate).astype(jnp.bfloat16)
        grad_value = dot_tn(weights, grad_mixed).astype(jnp.bfloat16).astype(jnp.float32)
        proj_grad[rows, width : 2 * width] = (grad_value * value_slope).astype(jnp.bfloat16)
        grad_weights = dot_nt(grad_mixed, value).astype(jnp.bfloat16).astype(jnp.float32)
        grad_scores = (grad_weights * raised * (2.0 * root / length)).astype(jnp.bfloat16)
        grad_query = jnp.dot(grad_scores, keyed, preferred_element_type=jnp.float32)
        grad_keyed = dot_tn(grad_scores, query)
        grad_query = grad_query.astype(jnp.bfloat16).astype(jnp.float32)
        grad_keyed = grad_keyed.astype(jnp.bfloat16).astype(jnp.float32)
        scale_sums[0] += jnp.sum(grad_query * mixed_in, axis=0, keepdims=True)
        scale_sums[1] += jnp.sum(grad_keyed * mixed_in, axis=0, keepdims=True)
        grad_shared = grad_query * first_scale + grad_keyed * second_scale
        proj_grad[rows, 2 * width :] = (grad_shared * mixed_slope).astype(jnp.bfloat16)
        between()
    chunk = 512
    for low in range(0, columns, chunk):
        high = min(low + chunk, columns)
        store_rows(in_grad, dot_tn(hidden_ref[...], proj_grad[:, low:high]), low, high)
    in_ready()
    between()
    small_all[...] = small[...]
    gain = gain_ref[...]
    gain_sum = 0.0
    for low in range(0, frames, length):
        rows = slice(low, low + length)
        grad_hidden = dot_nt(proj_grad[rows], win_ref[...])
        inputs = x_ref[rows].astype(jnp.float32)
        scaled = lax.rsqrt(jnp.mean(inputs * inputs, axis=-1, keepdims=True) + EPSILON)
        unit = inputs * scaled
        gain_sum += jnp.sum(grad_hidden * unit, axis=0, keepdims=True)
        pulled = grad_hidden * gain
        along = jnp.mean(pulled * unit, axis=-1, keepdims=True)
        back_ref[rows] = (
            up_ref[rows].astype(jnp.float32) + scaled * (pulled - unit * along)
        ).astype(jnp.bfloat16)
        between()
    lanes = gain.shape[-1] // 128
    for line in range(lanes):
        small_all[line : line + 1] = gain_sum[:, 128 * line : 128 * (line + 1)]
    small_all[2 * lanes : 2 * lanes + 1] = scale_sums[0]
    small_all[2 * lanes + 1 : 2 * lanes + 2] = scale_sums[1]


def reduced(partials, cuts, small, scaling, block=0, held_in=()):
    dp_bits, seq_bits = axis_bits("dp"), axis_bits("seq")
    steps = len(dp_bits) + len(seq_bits)
    shaped, shapes, accs, gathers, landings = [], [], [], [], []
    for partial in partials:
        rows, columns = partial.shape
        shaped.append(partial.reshape((2,) * steps + (rows >> steps, columns)))
    wide = [value.shape for value in shaped]
    made_here, back_shape = [], []
    if block:
        x, _, _, projected, _, _, weight_out, _, _ = held_in
        for rows, columns in (weight_out.shape, (x.shape[1], projected.shape[1])):
            wide.append((2,) * steps + (rows >> steps, columns))
        made_here = [pltpu.VMEM(shape, jnp.bfloat16) for shape in wide[-2:]]
        made_here.append(pltpu.VMEM(projected.shape, jnp.bfloat16))
        made_here.append(pltpu.VMEM((small.size // 128, 128), jnp.float32))
        back_shape = [jax.ShapeDtypeStruct(x.shape, jnp.bfloat16)]
    for shape in wide:
        shapes.append(
            jax.ShapeDtypeStruct((1 << len(seq_bits),) + shape[-2:], jnp.float32)
        )
    for array, low, high, _ in cuts:
        tail = (wide[array][-2], high - low)
        accs.append(pltpu.VMEM((2,) * (steps - 1) + tail, jnp.bfloat16))
        gathers.append(pltpu.VMEM((2,) * len(seq_bits) + tail, jnp.bfloat16))
        landings += [
            pltpu.VMEM((2,) * (steps - 1 - step) + tail, jnp.bfloat16) for step in range(steps)
        ]
    lines = small.reshape(-1, 128)
    sems = pltpu.SemaphoreType.DMA((len(cuts) + 1, steps + len(seq_bits)))
    space = pl.BlockSpec(memory_space=pltpu.VMEM)
    outs = shapes + [jax.ShapeDtypeStruct(lines.shape, jnp.float32)] + back_shape
    made = pl.pallas_call(
        partial_of(gradient_kernel, cuts, scaling, len(partials), block, len(held_in)),
        out_shape=outs,
        in_specs=[space] * (len(partials) + 1 + len(held_in)),
        out_specs=[space] * len(outs),
        scratch_shapes=[
            pltpu.VMEM((steps + 1,) + lines.shape, jnp.float32),
            pltpu.VMEM((steps,) + lines.shape, jnp.float32),
            sems,
            sems,
        ]
        + accs
        + gathers
        + landings
        + made_here,
        compiler_params=pltpu.CompilerParams(
            collective_id=0, has_side_effects=True, vmem_limit_bytes=56 << 20
        ),
        name="gradient_sums",
    )(*shaped, lines, *held_in)
    sums = [value.reshape(-1, value.shape[-1]) for value in made[: len(wide)]]
    return sums, made[len(wide)].reshape(-1), made[len(wide) + 1 :]


def exchange(value, split, join):
    count = lax.axis_size("seq")
    me = lax.axis_index("seq")
    piece = value.shape[split] // count
    width = value.shape[join]
    shape = list(value.shape)
    shape[split] = piece
    shape[join] = width * count
    out = jnp.zeros(shape, value.dtype)
    for step in range(count):
        other = jnp.bitwise_xor(me, step)
        part = lax.dynamic_slice_in_dim(value, other * piece, piece, split)
        if step:
            part = lax.ppermute(part, "seq", [(i, i ^ step) for i in range(count)])
        out = lax.dynamic_update_slice_in_dim(out, part, other * width, join)
    return out


def column_cuts(columns, parts):
    lanes = columns // 128
    ends = [128 * ((lanes * (i + 1)) // parts) for i in range(parts)]
    return list(zip([0] + ends[:-1], ends))


def on_device(frames, cotangent, weight_in, qk_scales, weight_out, gains):
    block_count = frames.shape[1] // BLOCK
    width = frames.shape[2]
    tokens_all = frames.shape[0] * frames.shape[1] * lax.axis_size("dp") * lax.axis_size("seq")
    scaling = tokens_all ** (-0.5)
    blocked = frames.reshape(-1, BLOCK, width)
    upstream = exchange(cotangent.reshape(block_count, BLOCK, width), 1, 0)
    first, saved_first = unit_forward(
        blocked, weight_in[0], qk_scales[0], weight_out[0], gains[0], 1
    )
    first_pos = exchange(first, 1, 0)
    second, saved_second = unit_forward(
        first_pos, weight_in[1], qk_scales[1], weight_out[1], gains[1], 0
    )
    result = exchange(second, 0, 1)
    back_pos, in_late, out_late, gain_late, scale_late = unit_backward(
        first_pos, upstream, weight_in[1], qk_scales[1], weight_out[1], gains[1], saved_second, 0
    )
    back_first = exchange(back_pos, 0, 1)
    steps = len(axis_bits("dp")) + len(axis_bits("seq"))
    fits = (width >> steps) % 16 == 0 and width % 128 == 0
    grads = [value.astype(jnp.bfloat16) for value in (in_late, out_late)]
    if fits:
        gain_early = jnp.zeros_like(gain_late)
        scale_early = jnp.zeros_like(scale_late)
    else:
        back_frames, in_early, out_early, gain_early, scale_early = unit_backward(
            blocked, back_first, weight_in[0], qk_scales[0], weight_out[0], gains[0], saved_first, 1
        )
        grads += [value.astype(jnp.bfloat16) for value in (out_early, in_early)]
    packed = jnp.concatenate(
        [gain_early, gain_late, scale_early.reshape(-1), scale_late.reshape(-1)]
    )
    cuts = []
    shapes = [weight_in.shape[2], width, width, weight_in.shape[2]]
    for array, (parts, turn) in enumerate(((3, 0), (3, 1), (2, 0), (3, 0))):
        for index, (low, high) in enumerate(column_cuts(shapes[array], parts)):
            cuts.append((array, low, high, turn + index))
    if fits:
        hidden, projected, gated = saved_first
        flat = [
            value.reshape(-1, value.shape[-1])
            for value in (blocked, back_first, hidden, projected, gated)
        ]
        held_in = flat + [weight_in[0], weight_out[0], qk_scales[0], gains[0:1]]
        sums, small, (back_frames,) = reduced(grads, cuts, packed, scaling, BLOCK, held_in)
    else:
        sums, small, _ = reduced(grads, cuts, packed, scaling)
    in_sum, out_sum = [sums[3], sums[0]], [sums[2], sums[1]]
    return (
        result.reshape(frames.shape),
        back_frames.reshape(frames.shape),
        jnp.stack(in_sum),
        jnp.stack(out_sum),
        small[: 2 * width].reshape(2, width),
        small[2 * width :].reshape(qk_scales.shape),
    )


def solution(mesh):
    in_specs = (P("dp", "seq", None), P("dp", "seq", None), P(), P(), P(), P())
    out_specs = (
        P("dp", "seq", None),
        P("dp", "seq", None),
        P(None, "dp", None),
        P(None, "dp", None),
        P(),
        P(),
    )
    return jax.shard_map(
        on_device, mesh=mesh, in_specs=in_specs, out_specs=out_specs, check_vma=False
    )
```

```python
from functools import partial
from functools import partial as partial_of

import jax
import jax.numpy as jnp
from jax import lax
from jax.experimental import pallas as pl
from jax.experimental.pallas import tpu as pltpu
from jax.sharding import PartitionSpec as P

BLOCK = 256


EPSILON = 1e-06


def normed(values, gain_row):
    scaling = lax.rsqrt(jnp.mean(values * values, axis=-1, keepdims=True) + EPSILON)
    return values * scaling * gain_row


def mixer(projected, scale_pair, attend_axis):
    width = (projected.shape[-1] - scale_pair.shape[-1]) // 2
    active = jax.nn.silu(projected)
    gate_part = active[..., :width]
    value_part = active[..., width : 2 * width].astype(jnp.bfloat16)
    shared = active[..., 2 * width :]
    query = (shared * scale_pair[0]).astype(jnp.bfloat16)
    keyed = (shared * scale_pair[1]).astype(jnp.bfloat16)
    length = projected.shape[attend_axis]
    if attend_axis == 1:
        score_form = "gls,gms->glm"
        mix_form = "glm,gme->gle"
    else:
        score_form = "lgs,mgs->glm"
        mix_form = "glm,mge->lge"
    scores = jnp.einsum(score_form, query, keyed, preferred_element_type=jnp.float32)
    scores = scores * scale_pair.shape[-1] ** (-0.5)
    weights = (jnp.square(jax.nn.relu(scores)) / length).astype(jnp.bfloat16)
    mixed = jnp.einsum(mix_form, weights, value_part, preferred_element_type=jnp.float32)
    return (gate_part * mixed).astype(jnp.bfloat16)


def rows_product(left, right):
    left_rows = left.reshape(-1, left.shape[-1])
    right_rows = right.reshape(-1, right.shape[-1])
    return lax.dot_general(
        left_rows, right_rows, (((0,), (0,)), ((), ())), preferred_element_type=jnp.float32
    )


def against(values, weight):
    return lax.dot_general(
        values, weight, (((values.ndim - 1,), (1,)), ((), ())), preferred_element_type=jnp.float32
    )


def unit_forward(inputs_now, weight_in, scale_pair, weight_out, gain_row, attend_axis):
    hidden = normed(inputs_now.astype(jnp.float32), gain_row).astype(jnp.bfloat16)
    projected = jnp.dot(hidden, weight_in, preferred_element_type=jnp.float32)
    gated = mixer(projected, scale_pair, attend_axis)
    result = (
        inputs_now.astype(jnp.float32)
        + jnp.dot(gated, weight_out, preferred_element_type=jnp.float32)
    ).astype(jnp.bfloat16)
    return (result, (hidden, projected, gated))


def unit_backward(
    inputs_now, upstream, weight_in, scale_pair, weight_out, gain_row, saved, attend_axis
):
    hidden, projected, gated = saved
    grad_out = rows_product(gated, upstream)
    grad_gated = against(upstream, weight_out).astype(jnp.bfloat16)
    pulled = jax.vjp(partial(mixer, attend_axis=attend_axis), projected, scale_pair)[1]
    grad_proj, grad_scale = pulled(grad_gated)
    grad_proj = grad_proj.astype(jnp.bfloat16)
    grad_in = rows_product(hidden, grad_proj)
    grad_hidden = against(grad_proj, weight_in)
    norm_pull = jax.vjp(normed, inputs_now.astype(jnp.float32), gain_row)[1]
    grad_inputs, grad_gain = norm_pull(grad_hidden)
    grad_inputs = (upstream.astype(jnp.float32) + grad_inputs).astype(jnp.bfloat16)
    return (grad_inputs, grad_in, grad_out, grad_gain, grad_scale)


def bit_of(axis, bit):
    return lax.rem(lax.axis_index(axis) // (1 << bit), 2)


def axis_bits(axis):
    return [(axis, bit) for bit in range(lax.axis_size(axis).bit_length() - 1)]


def partner(axis, bit):
    spot = {name: lax.axis_index(name) for name in ("dp", "seq")}
    spot[axis] = spot[axis] + (1 << bit) * (1 - 2 * bit_of(axis, bit))
    return (spot["dp"], spot["seq"])


def halving_order(turn):
    dp_bits, seq_bits = axis_bits("dp"), axis_bits("seq")
    rest = dp_bits[1:2] + seq_bits + dp_bits[2:-1]
    turn = turn % max(len(rest), 1)
    return dp_bits[:1] + rest[turn:] + rest[:turn] + dp_bits[2:][-1:]


def place_of(known, leading):
    return tuple(known.get(bit, slice(None)) for bit in leading)


SLOTS = ((0, 1), (1, 1), (1, 0), (0, 0))


def gradient_kernel(plan, scaling, count_in, block, count_held, *refs):
    dp_bits, seq_bits = axis_bits("dp"), axis_bits("seq")
    leading = dp_bits[::-1] + seq_bits[::-1]
    steps = len(leading)
    given, small = list(refs[:count_in]), refs[count_in]
    refs = list(refs[count_in + 1 :])
    held_in, refs = refs[:count_held], refs[count_held:]
    refs_of_scales = list(held_in[7:])
    results, small_out = refs[:2], refs[2]
    scratch = refs[3:]
    if block:
        back_ref, scratch = scratch[0], scratch[1:]
        out_grad, in_grad, proj_grad, small_all, proj_here, win_here, wout_here, load_sems = (
            scratch[-8:]
        )
        given += [out_grad, in_grad]
        scratch = scratch[:-8]
        x_ref, up_ref, hidden_ref, proj_ref, gated_ref, win_ref, wout_ref = held_in[:7]
        loads = [
            pltpu.make_async_copy(source, target, load_sems.at[spot])
            for spot, (source, target) in enumerate(
                (
                    (wout_ref.at[0], wout_here),
                    (proj_ref, proj_here),
                    (win_ref.at[0], win_here),
                )
            )
        ]
        for load in loads:
            load.start()
        held_in = [x_ref, up_ref, hidden_ref, proj_here, gated_ref, win_here, wout_here]
        held_in += refs_of_scales
    small_held, small_got, send_sems, recv_sems = scratch[:4]
    scratch = scratch[4:]
    total = len(plan)
    accs, scratch = scratch[:total], scratch[total:]
    gathers, scratch = scratch[:total], scratch[total:]
    landings = [scratch[steps * i : steps * (i + 1)] for i in range(total)]
    mine = {bit: bit_of(*bit) for bit in leading}
    where = {bit: partner(*bit) for bit in leading}
    barrier = pltpu.get_barrier_semaphore()
    for bit in leading:
        pl.semaphore_signal(
            barrier, inc=1, device_id=where[bit], device_id_type=pl.DeviceIdType.MESH
        )
    pl.semaphore_wait(barrier, steps)
    started = []

    def send(source, target, row, column, bit):
        copy = pltpu.make_async_remote_copy(
            src_ref=source,
            dst_ref=target,
            send_sem=send_sems.at[row, column],
            recv_sem=recv_sems.at[row, column],
            device_id=where[bit],
            device_id_type=pl.DeviceIdType.MESH,
        )
        copy.start()
        started.append(copy)
        return copy

    orders = [halving_order(turn) for _, _, _, turn in plan]
    flying = [None] * total
    known = [{} for _ in plan]

    def launch(index, step):
        array, low, high, _ = plan[index]
        bit = orders[index][step]
        if step == 0:
            left = leading
            place = place_of({bit: 1 - mine[bit]}, left)
            source = given[array].at[place + (slice(None), slice(low, high))]
        else:
            left = [other for other in leading if other != orders[index][0]]
            place = place_of({**known[index], bit: 1 - mine[bit]}, left)
            source = accs[index].at[place]
        flying[index] = send(source, landings[index][step], index, step, bit)

    at_step = [0] * total
    small_state = {"step": 0}

    def advance(index):
        step = at_step[index]
        if step >= steps:
            return
        array, low, high, _ = plan[index]
        bit = orders[index][step]
        flying[index].wait_recv()
        landed = landings[index][step]
        left = [other for other in leading if other != orders[index][0]]
        if step == 0:
            place = place_of({bit: mine[bit]}, leading)
            accs[index][...] = given[array][place + (slice(None), slice(low, high))] + landed[...]
        else:
            known[index][bit] = mine[bit]
            place = place_of(known[index], left)
            accs[index][place] = accs[index][place] + landed[...]
        at_step[index] = step + 1
        if step + 1 < steps:
            launch(index, step + 1)
        else:
            gathers[index][place_of(mine, seq_bits)] = accs[index][place_of(mine, left)]
            if seq_bits:
                spot = gathers[index].at[place_of(mine, seq_bits)]
                flying[index] = send(spot, spot, index, steps, seq_bits[0])

    def small_send():
        step = small_state["step"]
        small_state["copy"] = send(
            small_held.at[step], small_got.at[step], total, step, leading[step]
        )

    def small_advance():
        step = small_state["step"]
        if step >= steps:
            return
        small_state["copy"].wait_recv()
        small_held[step + 1] = small_held[step] + small_got[step]
        small_state["step"] = step + 1
        if step + 1 < steps:
            small_send()

    def of_arrays(*wanted):
        return [index for index in range(total) if plan[index][0] in wanted]

    def advance_all(*wanted):
        for index in of_arrays(*wanted):
            advance(index)

    def launch_all(*wanted):
        for index in of_arrays(*wanted):
            launch(index, 0)

    if block:
        late = tuple(range(count_in))
        out_at, in_at = count_in, count_in + 1
        launch_all(*late)
        block_backward(
            block,
            held_in,
            (back_ref, out_grad, in_grad, proj_grad, small_all),
            small,
            (
                lambda: launch_all(out_at),
                lambda: advance_all(*late),
                lambda: launch_all(in_at),
                [load.wait for load in loads],
            ),
        )
        small_held[0] = small_all[...]
    else:
        launch_all(*range(count_in))
        small_held[0] = small[...]
    small_send()
    while min(at_step) < steps:
        if block:
            advance_all(in_at)
            advance_all(*late, out_at)
        else:
            advance_all(*range(count_in))
        small_advance()
    while small_state["step"] < steps:
        small_advance()
    small_out[...] = small_held[steps] * scaling
    for turn in range(1, len(seq_bits)):
        for index in range(total):
            flying[index].wait_recv()
            have = {bit: mine[bit] for bit in seq_bits[turn:]}
            spot = gathers[index].at[place_of(have, seq_bits)]
            flying[index] = send(spot, spot, index, steps + turn, seq_bits[turn])
    for index in range(total):
        array, low, high, _ = plan[index]
        if seq_bits:
            flying[index].wait_recv()
        inner = gathers[index].shape[-2]
        for part in range(1 << len(seq_bits)):
            spot = tuple((part >> bit) % 2 for _, bit in seq_bits)
            place, unit = SLOTS[array]
            results[place][unit, part, :, low:high] = (
                gathers[index][spot].astype(jnp.float32) * scaling
            )
    for copy in started:
        copy.wait_send()


def dot_nt(left, right):
    return lax.dot_general(
        left, right, (((1,), (1,)), ((), ())), preferred_element_type=jnp.float32
    )


def dot_tn(left, right):
    return lax.dot_general(
        left, right, (((0,), (0,)), ((), ())), preferred_element_type=jnp.float32
    )


def silu_pair(values):
    sigmoid = 1.0 / (1.0 + jnp.exp(-values))
    active = values * sigmoid
    return active, sigmoid + active * (1.0 - sigmoid)


def store_rows(target, value, low, high):
    lead = target.shape[:-2]
    target[(slice(None),) * (len(lead) + 1) + (slice(low, high),)] = value.astype(
        jnp.bfloat16
    ).reshape(lead + (target.shape[-2], high - low))


def block_backward(length, held_in, made, small, hooks):
    x_ref, up_ref, hidden_ref, proj_ref, gated_ref, win_ref, wout_ref, scale_ref, gain_ref = held_in
    back_ref, out_grad, in_grad, proj_grad, small_all = made
    out_ready, between, in_ready, loaded = hooks
    frames, columns = proj_ref.shape
    shared = scale_ref.shape[-1]
    width = (columns - shared) // 2
    store_rows(out_grad, dot_tn(gated_ref[...], up_ref[...]), 0, up_ref.shape[-1])
    out_ready()
    between()
    loaded[0]()
    loaded[1]()
    root = shared ** (-0.5)
    first_scale, second_scale = scale_ref[0:1], scale_ref[1:2]
    scale_sums = [0.0, 0.0]
    for low in range(0, frames, length):
        rows = slice(low, low + length)
        grad_gated = dot_nt(up_ref[rows], wout_ref[...]).astype(jnp.bfloat16).astype(jnp.float32)
        mixed_in, mixed_slope = silu_pair(proj_ref[rows, 2 * width :])
        query = (mixed_in * first_scale).astype(jnp.bfloat16)
        keyed = (mixed_in * second_scale).astype(jnp.bfloat16)
        value, value_slope = silu_pair(proj_ref[rows, width : 2 * width])
        value = value.astype(jnp.bfloat16)
        raised = jnp.maximum(dot_nt(query, keyed) * root, 0.0)
        weights = (raised * raised / length).astype(jnp.bfloat16)
        mixed = jnp.dot(weights, value, preferred_element_type=jnp.float32)
        gate, gate_slope = silu_pair(proj_ref[rows, :width])
        proj_grad[rows, :width] = (grad_gated * mixed * gate_slope).astype(jnp.bfloat16)
        grad_mixed = (grad_gated * gate).astype(jnp.bfloat16)
        grad_value = dot_tn(weights, grad_mixed).astype(jnp.bfloat16).astype(jnp.float32)
        proj_grad[rows, width : 2 * width] = (grad_value * value_slope).astype(jnp.bfloat16)
        grad_weights = dot_nt(grad_mixed, value).astype(jnp.bfloat16).astype(jnp.float32)
        grad_scores = (grad_weights * raised * (2.0 * root / length)).astype(jnp.bfloat16)
        grad_query = jnp.dot(grad_scores, keyed, preferred_element_type=jnp.float32)
        grad_keyed = dot_tn(grad_scores, query)
        grad_query = grad_query.astype(jnp.bfloat16).astype(jnp.float32)
        grad_keyed = grad_keyed.astype(jnp.bfloat16).astype(jnp.float32)
        scale_sums[0] += jnp.sum(grad_query * mixed_in, axis=0, keepdims=True)
        scale_sums[1] += jnp.sum(grad_keyed * mixed_in, axis=0, keepdims=True)
        grad_shared = grad_query * first_scale + grad_keyed * second_scale
        proj_grad[rows, 2 * width :] = (grad_shared * mixed_slope).astype(jnp.bfloat16)
    between()
    chunk = 512
    for low in range(0, columns, chunk):
        high = min(low + chunk, columns)
        store_rows(in_grad, dot_tn(hidden_ref[...], proj_grad[:, low:high]), low, high)
    in_ready()
    loaded[2]()
    small_all[...] = small[...]
    gain = gain_ref[...]
    gain_sum = 0.0
    for low in range(0, frames, length):
        rows = slice(low, low + length)
        grad_hidden = dot_nt(proj_grad[rows], win_ref[...])
        inputs = x_ref[rows].astype(jnp.float32)
        scaled = lax.rsqrt(jnp.mean(inputs * inputs, axis=-1, keepdims=True) + EPSILON)
        unit = inputs * scaled
        gain_sum += jnp.sum(grad_hidden * unit, axis=0, keepdims=True)
        pulled = grad_hidden * gain
        along = jnp.mean(pulled * unit, axis=-1, keepdims=True)
        back_ref[rows] = (
            up_ref[rows].astype(jnp.float32) + scaled * (pulled - unit * along)
        ).astype(jnp.bfloat16)
    lanes = gain.shape[-1] // 128
    for line in range(lanes):
        small_all[line : line + 1] = gain_sum[:, 128 * line : 128 * (line + 1)]
    small_all[2 * lanes : 2 * lanes + 1] = scale_sums[0]
    small_all[2 * lanes + 1 : 2 * lanes + 2] = scale_sums[1]


def reduced(partials, cuts, small, scaling, block=0, held_in=()):
    dp_bits, seq_bits = axis_bits("dp"), axis_bits("seq")
    steps = len(dp_bits) + len(seq_bits)
    shaped, shapes, accs, gathers, landings = [], [], [], [], []
    for partial in partials:
        rows, columns = partial.shape
        shaped.append(partial.reshape((2,) * steps + (rows >> steps, columns)))
    wide = [value.shape for value in shaped]
    made_here, back_shape = [], []
    if block:
        x, _, _, projected, _, weight_in, weight_out, _, _ = held_in
        for rows, columns in (weight_out.shape[1:], weight_in.shape[1:]):
            wide.append((2,) * steps + (rows >> steps, columns))
        made_here = [pltpu.VMEM(shape, jnp.bfloat16) for shape in wide[-2:]]
        made_here.append(pltpu.VMEM(projected.shape, jnp.bfloat16))
        made_here.append(pltpu.VMEM((small.size // 128, 128), jnp.float32))
        made_here.append(pltpu.VMEM(projected.shape, jnp.float32))
        made_here += [pltpu.VMEM(w.shape[1:], jnp.bfloat16) for w in (weight_in, weight_out)]
        made_here.append(pltpu.SemaphoreType.DMA((3,)))
        back_shape = [jax.ShapeDtypeStruct(x.shape, jnp.bfloat16)]
    for shape in wide[:2]:
        shapes.append(
            jax.ShapeDtypeStruct((2, 1 << len(seq_bits)) + shape[-2:], jnp.float32)
        )
    for array, low, high, _ in cuts:
        tail = (wide[array][-2], high - low)
        accs.append(pltpu.VMEM((2,) * (steps - 1) + tail, jnp.bfloat16))
        gathers.append(pltpu.VMEM((2,) * len(seq_bits) + tail, jnp.bfloat16))
        landings += [
            pltpu.VMEM((2,) * (steps - 1 - step) + tail, jnp.bfloat16) for step in range(steps)
        ]
    limit = (40 if block else 24) << 20
    lines = small.reshape(-1, 128)
    sems = pltpu.SemaphoreType.DMA((len(cuts) + 1, steps + len(seq_bits)))
    space = pl.BlockSpec(memory_space=pltpu.VMEM)
    outs = shapes + [jax.ShapeDtypeStruct(lines.shape, jnp.float32)] + back_shape
    made = pl.pallas_call(
        partial_of(gradient_kernel, cuts, scaling, len(partials), block, len(held_in)),
        out_shape=outs,
        in_specs=[space] * (len(partials) + 1)
        + [
            pl.BlockSpec(memory_space=pl.ANY) if spot in (3, 5, 6) else space
            for spot in range(len(held_in))
        ],
        out_specs=[space] * len(outs),
        scratch_shapes=[
            pltpu.VMEM((steps + 1,) + lines.shape, jnp.float32),
            pltpu.VMEM((steps,) + lines.shape, jnp.float32),
            sems,
            sems,
        ]
        + accs
        + gathers
        + landings
        + made_here,
        compiler_params=pltpu.CompilerParams(
            collective_id=0, has_side_effects=True, vmem_limit_bytes=limit
        ),
        name="gradient_sums",
    )(*shaped, lines, *held_in)
    sums = [value.reshape(2, -1, value.shape[-1]) for value in made[:2]]
    return sums, made[2].reshape(-1), made[3:]


def exchange(value, split, join):
    count = lax.axis_size("seq")
    me = lax.axis_index("seq")
    piece = value.shape[split] // count
    width = value.shape[join]
    shape = list(value.shape)
    shape[split] = piece
    shape[join] = width * count
    if count == 2:
        halves = jnp.split(value, 2, axis=split)
        own = jnp.where(me == 0, halves[0], halves[1])
        got = lax.ppermute(jnp.where(me == 0, halves[1], halves[0]), "seq", [(0, 1), (1, 0)])
        return jnp.concatenate(
            [jnp.where(me == 0, own, got), jnp.where(me == 0, got, own)], axis=join
        )
    out = jnp.zeros(shape, value.dtype)
    for step in range(count):
        other = jnp.bitwise_xor(me, step)
        part = lax.dynamic_slice_in_dim(value, other * piece, piece, split)
        if step:
            part = lax.ppermute(part, "seq", [(i, i ^ step) for i in range(count)])
        out = lax.dynamic_update_slice_in_dim(out, part, other * width, join)
    return out


def column_cuts(columns, parts):
    lanes = columns // 128
    ends = [128 * ((lanes * (i + 1)) // parts) for i in range(parts)]
    return list(zip([0] + ends[:-1], ends))


def on_device(frames, cotangent, weight_in, qk_scales, weight_out, gains):
    block_count = frames.shape[1] // BLOCK
    width = frames.shape[2]
    tokens_all = frames.shape[0] * frames.shape[1] * lax.axis_size("dp") * lax.axis_size("seq")
    scaling = tokens_all ** (-0.5)
    blocked = frames.reshape(-1, BLOCK, width)
    upstream = exchange(cotangent.reshape(block_count, BLOCK, width), 1, 0)
    first, saved_first = unit_forward(
        blocked, weight_in[0], qk_scales[0], weight_out[0], gains[0], 1
    )
    first_pos = exchange(first, 1, 0)
    second, saved_second = unit_forward(
        first_pos, weight_in[1], qk_scales[1], weight_out[1], gains[1], 0
    )
    result = exchange(second, 0, 1)
    back_pos, in_late, out_late, gain_late, scale_late = unit_backward(
        first_pos, upstream, weight_in[1], qk_scales[1], weight_out[1], gains[1], saved_second, 0
    )
    back_first = exchange(back_pos, 0, 1)
    steps = len(axis_bits("dp")) + len(axis_bits("seq"))
    fits = (width >> steps) % 16 == 0 and width % 128 == 0
    grads = [value.astype(jnp.bfloat16) for value in (in_late, out_late)]
    if fits:
        gain_early = jnp.zeros_like(gain_late)
        scale_early = jnp.zeros_like(scale_late)
    else:
        back_frames, in_early, out_early, gain_early, scale_early = unit_backward(
            blocked, back_first, weight_in[0], qk_scales[0], weight_out[0], gains[0], saved_first, 1
        )
        grads += [value.astype(jnp.bfloat16) for value in (out_early, in_early)]
    packed = jnp.concatenate(
        [gain_early, gain_late, scale_early.reshape(-1), scale_late.reshape(-1)]
    )
    cuts = []
    shapes = [weight_in.shape[2], width, width, weight_in.shape[2]]
    for array, (parts, turn) in enumerate(((3, 0), (3, 1), (2, 0), (3, 0))):
        for index, (low, high) in enumerate(column_cuts(shapes[array], parts)):
            cuts.append((array, low, high, turn + index))
    if fits:
        hidden, projected, gated = saved_first
        flat = [
            value.reshape(-1, value.shape[-1])
            for value in (blocked, back_first, hidden, projected, gated)
        ]
        held_in = flat + [weight_in, weight_out, qk_scales[0], gains[0:1]]
        sums, small, (back_frames,) = reduced(grads, cuts, packed, scaling, BLOCK, held_in)
    else:
        sums, small, _ = reduced(grads, cuts, packed, scaling)
    return (
        result.reshape(frames.shape),
        back_frames.reshape(frames.shape),
        sums[0],
        sums[1],
        small[: 2 * width].reshape(2, width),
        small[2 * width :].reshape(qk_scales.shape),
    )


def solution(mesh):
    in_specs = (P("dp", "seq", None), P("dp", "seq", None), P(), P(), P(), P())
    out_specs = (
        P("dp", "seq", None),
        P("dp", "seq", None),
        P(None, "dp", None),
        P(None, "dp", None),
        P(),
        P(),
    )
    return jax.shard_map(
        on_device, mesh=mesh, in_specs=in_specs, out_specs=out_specs, check_vma=False
    )
```

```python
from functools import partial
from functools import partial as partial_of

import jax
import jax.numpy as jnp
from jax import lax
from jax.experimental import pallas as pl
from jax.experimental.pallas import tpu as pltpu
from jax.sharding import PartitionSpec as P

BLOCK = 256


EPSILON = 1e-06


def normed(values, gain_row):
    scaling = lax.rsqrt(jnp.mean(values * values, axis=-1, keepdims=True) + EPSILON)
    return values * scaling * gain_row


def mixer(projected, scale_pair, attend_axis):
    width = (projected.shape[-1] - scale_pair.shape[-1]) // 2
    active = jax.nn.silu(projected)
    gate_part = active[..., :width]
    value_part = active[..., width : 2 * width].astype(jnp.bfloat16)
    shared = active[..., 2 * width :]
    query = (shared * scale_pair[0]).astype(jnp.bfloat16)
    keyed = (shared * scale_pair[1]).astype(jnp.bfloat16)
    length = projected.shape[attend_axis]
    if attend_axis == 1:
        score_form = "gls,gms->glm"
        mix_form = "glm,gme->gle"
    else:
        score_form = "lgs,mgs->glm"
        mix_form = "glm,mge->lge"
    scores = jnp.einsum(score_form, query, keyed, preferred_element_type=jnp.float32)
    scores = scores * scale_pair.shape[-1] ** (-0.5)
    weights = (jnp.square(jax.nn.relu(scores)) / length).astype(jnp.bfloat16)
    mixed = jnp.einsum(mix_form, weights, value_part, preferred_element_type=jnp.float32)
    return (gate_part * mixed).astype(jnp.bfloat16)


def rows_product(left, right):
    left_rows = left.reshape(-1, left.shape[-1])
    right_rows = right.reshape(-1, right.shape[-1])
    return lax.dot_general(
        left_rows, right_rows, (((0,), (0,)), ((), ())), preferred_element_type=jnp.float32
    )


def against(values, weight):
    return lax.dot_general(
        values, weight, (((values.ndim - 1,), (1,)), ((), ())), preferred_element_type=jnp.float32
    )


def unit_forward(inputs_now, weight_in, scale_pair, weight_out, gain_row, attend_axis):
    hidden = normed(inputs_now.astype(jnp.float32), gain_row).astype(jnp.bfloat16)
    projected = jnp.dot(hidden, weight_in, preferred_element_type=jnp.float32)
    gated = mixer(projected, scale_pair, attend_axis)
    result = (
        inputs_now.astype(jnp.float32)
        + jnp.dot(gated, weight_out, preferred_element_type=jnp.float32)
    ).astype(jnp.bfloat16)
    return (result, (hidden, projected, gated))


def unit_backward(
    inputs_now, upstream, weight_in, scale_pair, weight_out, gain_row, saved, attend_axis
):
    hidden, projected, gated = saved
    grad_out = rows_product(gated, upstream)
    grad_gated = against(upstream, weight_out).astype(jnp.bfloat16)
    pulled = jax.vjp(partial(mixer, attend_axis=attend_axis), projected, scale_pair)[1]
    grad_proj, grad_scale = pulled(grad_gated)
    grad_proj = grad_proj.astype(jnp.bfloat16)
    grad_in = rows_product(hidden, grad_proj)
    grad_hidden = against(grad_proj, weight_in)
    norm_pull = jax.vjp(normed, inputs_now.astype(jnp.float32), gain_row)[1]
    grad_inputs, grad_gain = norm_pull(grad_hidden)
    grad_inputs = (upstream.astype(jnp.float32) + grad_inputs).astype(jnp.bfloat16)
    return (grad_inputs, grad_in, grad_out, grad_gain, grad_scale)


def bit_of(axis, bit):
    return lax.rem(lax.axis_index(axis) // (1 << bit), 2)


def axis_bits(axis):
    return [(axis, bit) for bit in range(lax.axis_size(axis).bit_length() - 1)]


def partner(axis, bit):
    spot = {name: lax.axis_index(name) for name in ("dp", "seq")}
    spot[axis] = spot[axis] + (1 << bit) * (1 - 2 * bit_of(axis, bit))
    return (spot["dp"], spot["seq"])


def halving_order(turn):
    dp_bits, seq_bits = axis_bits("dp"), axis_bits("seq")
    rest = dp_bits[1:2] + seq_bits + dp_bits[2:-1]
    turn = turn % max(len(rest), 1)
    return dp_bits[:1] + rest[turn:] + rest[:turn] + dp_bits[2:][-1:]


def place_of(known, leading):
    return tuple(known.get(bit, slice(None)) for bit in leading)


SLOTS = ((0, 1), (1, 1), (1, 0), (0, 0))


def gradient_kernel(plan, scaling, count_in, block, count_held, *refs):
    dp_bits, seq_bits = axis_bits("dp"), axis_bits("seq")
    leading = dp_bits[::-1] + seq_bits[::-1]
    steps = len(leading)
    given, small = list(refs[:count_in]), refs[count_in]
    refs = list(refs[count_in + 1 :])
    held_in, refs = refs[:count_held], refs[count_held:]
    refs_of_scales = list(held_in[7:])
    results, small_out = refs[:2], refs[2]
    scratch = refs[3:]
    if block:
        back_ref, scratch = scratch[0], scratch[1:]
        out_grad, in_grad, proj_grad, small_all, proj_here, win_here, wout_here, load_sems = (
            scratch[-8:]
        )
        given += [out_grad, in_grad]
        scratch = scratch[:-8]
        x_ref, up_ref, hidden_ref, proj_ref, gated_ref, win_ref, wout_ref = held_in[:7]
        loads = [
            pltpu.make_async_copy(source, target, load_sems.at[spot])
            for spot, (source, target) in enumerate(
                (
                    (wout_ref.at[0], wout_here),
                    (proj_ref, proj_here),
                    (win_ref.at[0], win_here),
                )
            )
        ]
        for load in loads:
            load.start()
        held_in = [x_ref, up_ref, hidden_ref, proj_here, gated_ref, win_here, wout_here]
        held_in += refs_of_scales
    small_held, small_got, send_sems, recv_sems = scratch[:4]
    scratch = scratch[4:]
    total = len(plan)
    accs, scratch = scratch[:total], scratch[total:]
    gathers, scratch = scratch[:total], scratch[total:]
    landings = [scratch[steps * i : steps * (i + 1)] for i in range(total)]
    mine = {bit: bit_of(*bit) for bit in leading}
    where = {bit: partner(*bit) for bit in leading}
    barrier = pltpu.get_barrier_semaphore()
    for bit in leading:
        pl.semaphore_signal(
            barrier, inc=1, device_id=where[bit], device_id_type=pl.DeviceIdType.MESH
        )
    pl.semaphore_wait(barrier, steps)
    started = []

    def send(source, target, row, column, bit):
        copy = pltpu.make_async_remote_copy(
            src_ref=source,
            dst_ref=target,
            send_sem=send_sems.at[row, column],
            recv_sem=recv_sems.at[row, column],
            device_id=where[bit],
            device_id_type=pl.DeviceIdType.MESH,
        )
        copy.start()
        started.append(copy)
        return copy

    orders = [halving_order(turn) for _, _, _, turn in plan]
    flying = [None] * total
    known = [{} for _ in plan]

    def launch(index, step):
        array, low, high, _ = plan[index]
        bit = orders[index][step]
        if step == 0:
            left = leading
            place = place_of({bit: 1 - mine[bit]}, left)
            source = given[array].at[place + (slice(None), slice(low, high))]
        else:
            left = [other for other in leading if other != orders[index][0]]
            place = place_of({**known[index], bit: 1 - mine[bit]}, left)
            source = accs[index].at[place]
        flying[index] = send(source, landings[index][step], index, step, bit)

    at_step = [0] * total
    small_state = {"step": 0}

    def advance(index):
        step = at_step[index]
        if step >= steps:
            return
        array, low, high, _ = plan[index]
        bit = orders[index][step]
        flying[index].wait_recv()
        landed = landings[index][step]
        left = [other for other in leading if other != orders[index][0]]
        if step == 0:
            place = place_of({bit: mine[bit]}, leading)
            accs[index][...] = given[array][place + (slice(None), slice(low, high))] + landed[...]
        else:
            known[index][bit] = mine[bit]
            place = place_of(known[index], left)
            accs[index][place] = accs[index][place] + landed[...]
        at_step[index] = step + 1
        if step + 1 < steps:
            launch(index, step + 1)
        else:
            gathers[index][place_of(mine, seq_bits)] = accs[index][place_of(mine, left)]
            if seq_bits:
                spot = gathers[index].at[place_of(mine, seq_bits)]
                flying[index] = send(spot, spot, index, steps, seq_bits[0])

    def small_send():
        step = small_state["step"]
        small_state["copy"] = send(
            small_held.at[step], small_got.at[step], total, step, leading[step]
        )

    def small_advance():
        step = small_state["step"]
        if step >= steps:
            return
        small_state["copy"].wait_recv()
        small_held[step + 1] = small_held[step] + small_got[step]
        small_state["step"] = step + 1
        if step + 1 < steps:
            small_send()

    def of_arrays(*wanted):
        return [index for index in range(total) if plan[index][0] in wanted]

    def advance_all(*wanted):
        for index in of_arrays(*wanted):
            advance(index)

    def launch_all(*wanted):
        for index in of_arrays(*wanted):
            launch(index, 0)

    if block:
        late = tuple(range(count_in))
        out_at, in_at = count_in, count_in + 1
        launch_all(*late)
        block_backward(
            block,
            held_in,
            (back_ref, out_grad, in_grad, proj_grad, small_all),
            small,
            (
                lambda: launch_all(out_at),
                lambda *arrays: [advance_all(*part) for part in (arrays, late)],
                lambda: launch_all(in_at),
                [load.wait for load in loads],
            ),
        )
        small_held[0] = small_all[...]
    else:
        launch_all(*range(count_in))
        small_held[0] = small[...]
    small_send()
    while min(at_step) < steps:
        if block:
            advance_all(in_at)
            advance_all(*late, out_at)
        else:
            advance_all(*range(count_in))
        small_advance()
    while small_state["step"] < steps:
        small_advance()
    small_out[...] = small_held[steps] * scaling
    for turn in range(1, len(seq_bits)):
        for index in range(total):
            flying[index].wait_recv()
            have = {bit: mine[bit] for bit in seq_bits[turn:]}
            spot = gathers[index].at[place_of(have, seq_bits)]
            flying[index] = send(spot, spot, index, steps + turn, seq_bits[turn])
    for index in range(total):
        array, low, high, _ = plan[index]
        if seq_bits:
            flying[index].wait_recv()
        inner = gathers[index].shape[-2]
        for part in range(1 << len(seq_bits)):
            spot = tuple((part >> bit) % 2 for _, bit in seq_bits)
            place, unit = SLOTS[array]
            results[place][unit, part, :, low:high] = (
                gathers[index][spot].astype(jnp.float32) * scaling
            )
    for copy in started:
        copy.wait_send()


def dot_nt(left, right):
    return lax.dot_general(
        left, right, (((1,), (1,)), ((), ())), preferred_element_type=jnp.float32
    )


def dot_tn(left, right):
    return lax.dot_general(
        left, right, (((0,), (0,)), ((), ())), preferred_element_type=jnp.float32
    )


def silu_pair(values):
    sigmoid = 1.0 / (1.0 + jnp.exp(-values))
    active = values * sigmoid
    return active, sigmoid + active * (1.0 - sigmoid)


def store_rows(target, value, low, high):
    lead = target.shape[:-2]
    target[(slice(None),) * (len(lead) + 1) + (slice(low, high),)] = value.astype(
        jnp.bfloat16
    ).reshape(lead + (target.shape[-2], high - low))


def block_backward(length, held_in, made, small, hooks):
    x_ref, up_ref, hidden_ref, proj_ref, gated_ref, win_ref, wout_ref, scale_ref, gain_ref = held_in
    back_ref, out_grad, in_grad, proj_grad, small_all = made
    out_ready, between, in_ready, loaded = hooks
    frames, columns = proj_ref.shape
    shared = scale_ref.shape[-1]
    width = (columns - shared) // 2
    store_rows(out_grad, dot_tn(gated_ref[...], up_ref[...]), 0, up_ref.shape[-1])
    out_ready()
    between()
    loaded[0]()
    loaded[1]()
    root = shared ** (-0.5)
    first_scale, second_scale = scale_ref[0:1], scale_ref[1:2]
    scale_sums = [0.0, 0.0]
    for low in range(0, frames, length):
        rows = slice(low, low + length)
        grad_gated = dot_nt(up_ref[rows], wout_ref[...]).astype(jnp.bfloat16).astype(jnp.float32)
        mixed_in, mixed_slope = silu_pair(proj_ref[rows, 2 * width :])
        query = (mixed_in * first_scale).astype(jnp.bfloat16)
        keyed = (mixed_in * second_scale).astype(jnp.bfloat16)
        value, value_slope = silu_pair(proj_ref[rows, width : 2 * width])
        value = value.astype(jnp.bfloat16)
        raised = jnp.maximum(dot_nt(query, keyed) * root, 0.0)
        weights = (raised * raised / length).astype(jnp.bfloat16)
        mixed = jnp.dot(weights, value, preferred_element_type=jnp.float32)
        gate, gate_slope = silu_pair(proj_ref[rows, :width])
        proj_grad[rows, :width] = (grad_gated * mixed * gate_slope).astype(jnp.bfloat16)
        grad_mixed = (grad_gated * gate).astype(jnp.bfloat16)
        grad_value = dot_tn(weights, grad_mixed).astype(jnp.bfloat16).astype(jnp.float32)
        proj_grad[rows, width : 2 * width] = (grad_value * value_slope).astype(jnp.bfloat16)
        grad_weights = dot_nt(grad_mixed, value).astype(jnp.bfloat16).astype(jnp.float32)
        grad_scores = (grad_weights * raised * (2.0 * root / length)).astype(jnp.bfloat16)
        grad_query = jnp.dot(grad_scores, keyed, preferred_element_type=jnp.float32)
        grad_keyed = dot_tn(grad_scores, query)
        grad_query = grad_query.astype(jnp.bfloat16).astype(jnp.float32)
        grad_keyed = grad_keyed.astype(jnp.bfloat16).astype(jnp.float32)
        scale_sums[0] += jnp.sum(grad_query * mixed_in, axis=0, keepdims=True)
        scale_sums[1] += jnp.sum(grad_keyed * mixed_in, axis=0, keepdims=True)
        grad_shared = grad_query * first_scale + grad_keyed * second_scale
        proj_grad[rows, 2 * width :] = (grad_shared * mixed_slope).astype(jnp.bfloat16)
    between(len(SLOTS) - 2)
    chunk = 512
    for low in range(0, columns, chunk):
        high = min(low + chunk, columns)
        store_rows(in_grad, dot_tn(hidden_ref[...], proj_grad[:, low:high]), low, high)
    in_ready()
    loaded[2]()
    small_all[...] = small[...]
    gain = gain_ref[...]
    gain_sum = 0.0
    for low in range(0, frames, length):
        rows = slice(low, low + length)
        grad_hidden = dot_nt(proj_grad[rows], win_ref[...])
        inputs = x_ref[rows].astype(jnp.float32)
        scaled = lax.rsqrt(jnp.mean(inputs * inputs, axis=-1, keepdims=True) + EPSILON)
        unit = inputs * scaled
        gain_sum += jnp.sum(grad_hidden * unit, axis=0, keepdims=True)
        pulled = grad_hidden * gain
        along = jnp.mean(pulled * unit, axis=-1, keepdims=True)
        back_ref[rows] = (
            up_ref[rows].astype(jnp.float32) + scaled * (pulled - unit * along)
        ).astype(jnp.bfloat16)
    lanes = gain.shape[-1] // 128
    for line in range(lanes):
        small_all[line : line + 1] = gain_sum[:, 128 * line : 128 * (line + 1)]
    small_all[2 * lanes : 2 * lanes + 1] = scale_sums[0]
    small_all[2 * lanes + 1 : 2 * lanes + 2] = scale_sums[1]


def reduced(partials, cuts, small, scaling, block=0, held_in=()):
    dp_bits, seq_bits = axis_bits("dp"), axis_bits("seq")
    steps = len(dp_bits) + len(seq_bits)
    shaped, shapes, accs, gathers, landings = [], [], [], [], []
    for partial in partials:
        rows, columns = partial.shape
        shaped.append(partial.reshape((2,) * steps + (rows >> steps, columns)))
    wide = [value.shape for value in shaped]
    made_here, back_shape = [], []
    if block:
        x, _, _, projected, _, weight_in, weight_out, _, _ = held_in
        for rows, columns in (weight_out.shape[1:], weight_in.shape[1:]):
            wide.append((2,) * steps + (rows >> steps, columns))
        made_here = [pltpu.VMEM(shape, jnp.bfloat16) for shape in wide[-2:]]
        made_here.append(pltpu.VMEM(projected.shape, jnp.bfloat16))
        made_here.append(pltpu.VMEM((small.size // 128, 128), jnp.float32))
        made_here.append(pltpu.VMEM(projected.shape, jnp.float32))
        made_here += [pltpu.VMEM(w.shape[1:], jnp.bfloat16) for w in (weight_in, weight_out)]
        made_here.append(pltpu.SemaphoreType.DMA((3,)))
        back_shape = [jax.ShapeDtypeStruct(x.shape, jnp.bfloat16)]
    for shape in wide[:2]:
        shapes.append(
            jax.ShapeDtypeStruct((2, 1 << len(seq_bits)) + shape[-2:], jnp.float32)
        )
    for array, low, high, _ in cuts:
        tail = (wide[array][-2], high - low)
        accs.append(pltpu.VMEM((2,) * (steps - 1) + tail, jnp.bfloat16))
        gathers.append(pltpu.VMEM((2,) * len(seq_bits) + tail, jnp.bfloat16))
        landings += [
            pltpu.VMEM((2,) * (steps - 1 - step) + tail, jnp.bfloat16) for step in range(steps)
        ]
    limit = (40 if block else 24) << 20
    lines = small.reshape(-1, 128)
    sems = pltpu.SemaphoreType.DMA((len(cuts) + 1, steps + len(seq_bits)))
    space = pl.BlockSpec(memory_space=pltpu.VMEM)
    outs = shapes + [jax.ShapeDtypeStruct(lines.shape, jnp.float32)] + back_shape
    made = pl.pallas_call(
        partial_of(gradient_kernel, cuts, scaling, len(partials), block, len(held_in)),
        out_shape=outs,
        in_specs=[space] * (len(partials) + 1)
        + [
            pl.BlockSpec(memory_space=pl.ANY) if spot in (3, 5, 6) else space
            for spot in range(len(held_in))
        ],
        out_specs=[space] * len(outs),
        scratch_shapes=[
            pltpu.VMEM((steps + 1,) + lines.shape, jnp.float32),
            pltpu.VMEM((steps,) + lines.shape, jnp.float32),
            sems,
            sems,
        ]
        + accs
        + gathers
        + landings
        + made_here,
        compiler_params=pltpu.CompilerParams(
            collective_id=0, has_side_effects=True, vmem_limit_bytes=limit
        ),
        name="gradient_sums",
    )(*shaped, lines, *held_in)
    sums = [value.reshape(2, -1, value.shape[-1]) for value in made[:2]]
    return sums, made[2].reshape(-1), made[3:]


def exchange(value, split, join):
    count = lax.axis_size("seq")
    me = lax.axis_index("seq")
    piece = value.shape[split] // count
    width = value.shape[join]
    shape = list(value.shape)
    shape[split] = piece
    shape[join] = width * count
    if count == 2:
        halves = jnp.split(value, 2, axis=split)
        own = jnp.where(me == 0, halves[0], halves[1])
        got = lax.ppermute(jnp.where(me == 0, halves[1], halves[0]), "seq", [(0, 1), (1, 0)])
        return jnp.concatenate(
            [jnp.where(me == 0, own, got), jnp.where(me == 0, got, own)], axis=join
        )
    out = jnp.zeros(shape, value.dtype)
    for step in range(count):
        other = jnp.bitwise_xor(me, step)
        part = lax.dynamic_slice_in_dim(value, other * piece, piece, split)
        if step:
            part = lax.ppermute(part, "seq", [(i, i ^ step) for i in range(count)])
        out = lax.dynamic_update_slice_in_dim(out, part, other * width, join)
    return out


def column_cuts(columns, parts):
    lanes = columns // 128
    ends = [128 * ((lanes * (i + 1)) // parts) for i in range(parts)]
    return list(zip([0] + ends[:-1], ends))


def on_device(frames, cotangent, weight_in, qk_scales, weight_out, gains):
    block_count = frames.shape[1] // BLOCK
    width = frames.shape[2]
    tokens_all = frames.shape[0] * frames.shape[1] * lax.axis_size("dp") * lax.axis_size("seq")
    scaling = tokens_all ** (-0.5)
    blocked = frames.reshape(-1, BLOCK, width)
    upstream = exchange(cotangent.reshape(block_count, BLOCK, width), 1, 0)
    first, saved_first = unit_forward(
        blocked, weight_in[0], qk_scales[0], weight_out[0], gains[0], 1
    )
    first_pos = exchange(first, 1, 0)
    second, saved_second = unit_forward(
        first_pos, weight_in[1], qk_scales[1], weight_out[1], gains[1], 0
    )
    result = exchange(second, 0, 1)
    back_pos, in_late, out_late, gain_late, scale_late = unit_backward(
        first_pos, upstream, weight_in[1], qk_scales[1], weight_out[1], gains[1], saved_second, 0
    )
    back_first = exchange(back_pos, 0, 1)
    steps = len(axis_bits("dp")) + len(axis_bits("seq"))
    fits = (width >> steps) % 16 == 0 and width % 128 == 0
    grads = [value.astype(jnp.bfloat16) for value in (in_late, out_late)]
    if fits:
        gain_early = jnp.zeros_like(gain_late)
        scale_early = jnp.zeros_like(scale_late)
    else:
        back_frames, in_early, out_early, gain_early, scale_early = unit_backward(
            blocked, back_first, weight_in[0], qk_scales[0], weight_out[0], gains[0], saved_first, 1
        )
        grads += [value.astype(jnp.bfloat16) for value in (out_early, in_early)]
    packed = jnp.concatenate(
        [gain_early, gain_late, scale_early.reshape(-1), scale_late.reshape(-1)]
    )
    cuts = []
    shapes = [weight_in.shape[2], width, width, weight_in.shape[2]]
    for array, (parts, turn) in enumerate(((3, 0), (3, 1), (2, 2), (3, 0))):
        for index, (low, high) in enumerate(column_cuts(shapes[array], parts)):
            cuts.append((array, low, high, turn + index))
    if fits:
        hidden, projected, gated = saved_first
        flat = [
            value.reshape(-1, value.shape[-1])
            for value in (blocked, back_first, hidden, projected, gated)
        ]
        held_in = flat + [weight_in, weight_out, qk_scales[0], gains[0:1]]
        sums, small, (back_frames,) = reduced(grads, cuts, packed, scaling, BLOCK, held_in)
    else:
        sums, small, _ = reduced(grads, cuts, packed, scaling)
    return (
        result.reshape(frames.shape),
        back_frames.reshape(frames.shape),
        sums[0],
        sums[1],
        small[: 2 * width].reshape(2, width),
        small[2 * width :].reshape(qk_scales.shape),
    )


def solution(mesh):
    in_specs = (P("dp", "seq", None), P("dp", "seq", None), P(), P(), P(), P())
    out_specs = (
        P("dp", "seq", None),
        P("dp", "seq", None),
        P(None, "dp", None),
        P(None, "dp", None),
        P(),
        P(),
    )
    return jax.shard_map(
        on_device, mesh=mesh, in_specs=in_specs, out_specs=out_specs, check_vma=False
    )
```
